32 devices in a mesh: pair: 2 (over x), seq: 8 (over z, y), head: 2 (over core).
Axes of the slice: x: 2, y: 2, z: 4, core: 2. Of those that a mesh axis runs over, the one named last changes fastest.
Arguments:
- queries: bfloat16 [2, 512, 2, 3584], P('pair', 'seq', None, 'head'), may hold values from -6 to 6
- answer_keys: bfloat16 [2, 512, 2, 512], P('pair', 'seq', None, 'head'), may hold values from -6 to 6
- answer_values: bfloat16 [2, 512, 2, 512], P('pair', 'seq', None, 'head'), may hold values from -6 to 6
- prefix_keys: bfloat16 [768, 512], P(('pair', 'seq'), 'head'), may hold values from -8 to 8
- prefix_values: bfloat16 [768, 512], P(('pair', 'seq'), 'head'), may hold values from -6 to 6
- grad_out: bfloat16 [2, 512, 2, 3584], P('pair', 'seq', None, 'head'), may hold values from -6 to 6
- answer_length: int32 [2, 2], P('pair'), may hold values from 128 to 512
- prefix_limit: int32 [2, 2], P('pair'), may hold values from 384 to 768
Outputs:
- attention_out: bfloat16 [2, 512, 2, 3584], P('pair', 'seq', None, 'head')
- grad_queries: bfloat16 [2, 512, 2, 3584], P('pair', 'seq', None, 'head')
- grad_answer_keys: bfloat16 [2, 512, 2, 512], P('pair', 'seq', None, 'head')
- grad_answer_values: bfloat16 [2, 512, 2, 512], P('pair', 'seq', None, 'head')
- grad_prefix_keys: float32 [768, 512], P(('pair', 'seq'), 'head')
- grad_prefix_values: float32 [768, 512], P(('pair', 'seq'), 'head')
The draws below stay inside these ranges and needn't reach their ends.
All inputs are finite; a program needn't handle non-finite values.
Results may differ from the reference program's by a relative error of at most 0.015.
Values may be sent and summed in bfloat16 or wider, within the bound.
A program may use at most 64 MiB of HBM per device.

```python
from functools import partial
import jax
import jax.numpy as jnp
from jax import lax

HEADS = 28
KV_HEADS = 4
HEAD_DIM = 128
BATCH = 2
ANS = 512
PREFIX = 768


def draw_queries(key, part):
    shape = (2, ANS, BATCH, HEADS * HEAD_DIM)
    values = jax.random.normal(jax.random.fold_in(key, 11), shape, jnp.float32)
    return jnp.clip(values, -6.0, 6.0).astype(jnp.bfloat16)


def draw_prefix_keys(key, part):
    shape = (PREFIX, KV_HEADS * HEAD_DIM)
    values = jax.random.normal(jax.random.fold_in(key, 13), shape, jnp.float32)
    return jnp.clip(values, -6.0, 6.0).astype(jnp.bfloat16)


def plant(values, rng, smallest, high):
    longest = values.shape.index(max(values.shape))
    spots = []
    for shift in (0, 1):
        where = [jax.random.randint(jax.random.fold_in(rng, axis), (), 0, length) for axis, length in enumerate(values.shape)]
        where[longest] = (where[longest] + shift) % values.shape[longest]
        spots.append(tuple(where))
    return values.at[spots[0]].set(smallest).at[spots[1]].set(high)


def levels(own_key, dims, split, smallest, top_value):
    def one(position, blocks):
        heights = jax.random.uniform(jax.random.fold_in(jax.random.fold_in(own_key, 6), position), (blocks,), jnp.float32, smallest / len(split), top_value / len(split))
        return jnp.repeat(jnp.exp(heights), dims[position] // blocks).reshape((-1,) + (1,) * (len(dims) - position - 1))

    gain = one(*split[0])
    for cut in split[1:]:
        gain = gain * one(*cut)
    return gain


def gaussian(rng, dims, scale, limit, split=(), kind=jnp.bfloat16):
    values = jax.random.normal(rng, dims, jnp.float32) * scale
    if len(split) > 0:
        values = levels(rng, dims, split, -0.22, 0.18) * values
    return jnp.clip(values, min=-limit, max=limit).astype(kind)


def setup_inputs(seed: int = 0) -> dict:
    keys = jax.random.split(jax.random.key(seed), 9)
    return {
        "queries": draw_queries(jax.random.fold_in(keys[8], 71), 0),
        "answer_keys": gaussian(keys[1], (2, ANS, BATCH, KV_HEADS * HEAD_DIM), 1.0, 6.0, ((0, 2), (1, 8), (3, 2))),
        "answer_values": gaussian(keys[2], (2, ANS, BATCH, KV_HEADS * HEAD_DIM), 1.0, 6.0, ((0, 2), (1, 8), (3, 2))),
        "prefix_keys": draw_prefix_keys(jax.random.fold_in(keys[8], 71), 0),
        "prefix_values": gaussian(keys[4], (PREFIX, KV_HEADS * HEAD_DIM), 1.0, 6.0, ((0, 16), (1, 2))),
        "grad_out": gaussian(keys[5], (2, ANS, BATCH, HEADS * HEAD_DIM), 1.0, 6.0, ((0, 2), (1, 8), (3, 2))),
        "answer_length": plant(jax.random.randint(keys[6], (2, BATCH), ANS // 4, ANS + 1), jax.random.fold_in(keys[6], 1), ANS // 4, ANS).astype(jnp.int32),
        "prefix_limit": plant(jax.random.randint(keys[7], (2, BATCH), PREFIX // 2, PREFIX + 1), jax.random.fold_in(keys[7], 1), PREFIX // 2, PREFIX).astype(jnp.int32),
    }


negative_fill = -1e30


def one_head(pair_items, keys_all, values_all, limit_here, length):
    head_queries, head_douts = pair_items
    scaling = HEAD_DIM ** -0.5
    raw_scores = jnp.dot(head_queries, keys_all.T, preferred_element_type=jnp.float32) * scaling
    columns = jnp.arange(PREFIX + ANS, dtype=jnp.int32)[None, :]
    positions = jnp.arange(ANS, dtype=jnp.int32)[:, None]
    allowed = jnp.where(columns < PREFIX, columns < limit_here, columns - PREFIX <= positions)
    masked = jnp.where(allowed, raw_scores, negative_fill)
    top_score = jnp.max(masked, axis=1, keepdims=True)
    exp_total = jnp.sum(jnp.where(allowed, jnp.exp(masked - top_score), 0.0), axis=1, keepdims=True)
    log_total = top_score + jnp.log(exp_total)
    probs = jnp.where(allowed, jnp.exp(raw_scores - log_total), 0.0)
    probs_low = lax.optimization_barrier(probs.astype(jnp.bfloat16))
    live = positions < length
    attended = jnp.where(live, jnp.dot(probs_low, values_all, preferred_element_type=jnp.float32), 0.0)
    douts = jnp.where(live, head_douts, jnp.zeros_like(head_douts))
    grad_probs = jnp.dot(douts, values_all.T, preferred_element_type=jnp.float32)
    delta = jnp.sum(douts.astype(jnp.float32) * attended, axis=1, keepdims=True)
    grad_low = lax.optimization_barrier((probs * (grad_probs - delta)).astype(jnp.bfloat16))
    grad_queries = jnp.dot(grad_low, keys_all, preferred_element_type=jnp.float32) * scaling
    key_terms = jnp.dot(grad_low.T, head_queries, preferred_element_type=jnp.float32) * scaling
    value_terms = jnp.dot(probs_low.T, douts, preferred_element_type=jnp.float32)
    return attended.astype(jnp.bfloat16), grad_queries.astype(jnp.bfloat16), key_terms, value_terms


def reference(queries, answer_keys, answer_values, prefix_keys, prefix_values, grad_out, answer_length, prefix_limit):
    group_size = HEADS // KV_HEADS
    group_width = group_size * HEAD_DIM
    prefix_key_sums = [jnp.zeros((PREFIX, HEAD_DIM), jnp.float32) for head_index in range(KV_HEADS)]
    prefix_value_sums = [jnp.zeros((PREFIX, HEAD_DIM), jnp.float32) for head_index in range(KV_HEADS)]
    out_sides, query_sides, key_sides, value_sides = [], [], [], []
    for side_index in range(2):
        out_items, query_items, key_items, value_items = [], [], [], []
        for answer_index in range(BATCH):
            out_heads, query_heads, key_heads, value_heads = [], [], [], []
            for head_index in range(KV_HEADS):
                key_columns = slice(head_index * HEAD_DIM, (head_index + 1) * HEAD_DIM)
                query_columns = slice(head_index * group_width, (head_index + 1) * group_width)
                keys_all = jnp.concatenate([prefix_keys[:, key_columns], answer_keys[side_index, :, answer_index, key_columns]], axis=0)
                values_all = jnp.concatenate([prefix_values[:, key_columns], answer_values[side_index, :, answer_index, key_columns]], axis=0)
                head_queries = queries[side_index, :, answer_index, query_columns].reshape(ANS, group_size, HEAD_DIM).transpose(1, 0, 2)
                head_douts = grad_out[side_index, :, answer_index, query_columns].reshape(ANS, group_size, HEAD_DIM).transpose(1, 0, 2)
                results = lax.map(partial(one_head, keys_all=keys_all, values_all=values_all, limit_here=prefix_limit[side_index, answer_index], length=answer_length[side_index, answer_index]), (head_queries, head_douts))
                out_heads.append(results[0].transpose(1, 0, 2).reshape(ANS, group_width))
                query_heads.append(results[1].transpose(1, 0, 2).reshape(ANS, group_width))
                key_total = jnp.sum(results[2], axis=0)
                value_total = jnp.sum(results[3], axis=0)
                prefix_key_sums[head_index] = prefix_key_sums[head_index] + key_total[:PREFIX]
                prefix_value_sums[head_index] = prefix_value_sums[head_index] + value_total[:PREFIX]
                key_heads.append(key_total[PREFIX:].astype(jnp.bfloat16))
                value_heads.append(value_total[PREFIX:].astype(jnp.bfloat16))
            out_items.append(jnp.concatenate(out_heads, axis=1))
            query_items.append(jnp.concatenate(query_heads, axis=1))
            key_items.append(jnp.concatenate(key_heads, axis=1))
            value_items.append(jnp.concatenate(value_heads, axis=1))
        out_sides.append(jnp.stack(out_items, axis=1))
        query_sides.append(jnp.stack(query_items, axis=1))
        key_sides.append(jnp.stack(key_items, axis=1))
        value_sides.append(jnp.stack(value_items, axis=1))
    return (jnp.stack(out_sides), jnp.stack(query_sides), jnp.stack(key_sides), jnp.stack(value_sides), jnp.concatenate(prefix_key_sums, axis=1), jnp.concatenate(prefix_value_sums, axis=1))
```

```python
import functools
import math

import jax
import jax.numpy as jnp
from jax import lax
from jax.experimental import pallas as pl
from jax.experimental.pallas import tpu as pltpu
from jax.sharding import PartitionSpec as P

HEAD_DIM = 128
FILL = -1e30
VM = pltpu.VMEM


def split_seq(seq_size):
    inner = 2 if seq_size % 2 == 0 else 1
    return seq_size // inner, inner


def place(pair_size, seq_size):
    outer, inner = split_seq(seq_size)
    p = lax.axis_index("pair")
    s = lax.axis_index("seq")
    z, y = s // inner, s % inner
    return outer, inner, p, s, z, y


def greet(pair_size, outer, inner, p, z, y):
    barrier = pltpu.get_barrier_semaphore()
    for j in range(1, pair_size):
        pl.semaphore_signal(barrier, inc=1, device_id={"pair": (p + j) % pair_size})
    for j in range(1, inner):
        pl.semaphore_signal(barrier, inc=1, device_id={"seq": z * inner + (y + j) % inner})
    for k in range(1, outer):
        pl.semaphore_signal(barrier, inc=1, device_id={"seq": ((z + k) % outer) * inner + y})


def greeted(pair_size, outer, inner):
    pl.semaphore_wait(pltpu.get_barrier_semaphore(), pair_size + inner + outer - 3)


def only(when, act):
    if when is None:
        act()
    else:
        pl.when(when)(act)


def chunks_of(slots, most):
    size = math.gcd(slots, most)
    return [(low, low + size) for low in range(0, slots, size)]


def flat_rows(block):
    return block.reshape(block.shape[0] * block.shape[1], block.shape[2])


def layer_kernel(
    pair_size, seq_size, batch, kv_heads, group,
    limits, lengths, q_ref, d_ref, ak_in, av_in, pk_in, pv_in,
    out_ref, dq_ref, ak_ref, av_ref, pk_ref, pv_ref,
    a_in, p_in, a_g, p_g, at_ref, pt_ref, e_ref, low_ref, acc_ref,
    rx, ry_p, rz_p, ry_a, rz_a, sy_p, sz_p, sz_a, own_a, own_p, q_s, d_s, o_s,
    gaz_s, gaz_r, gpz_s, gpz_r, gay_s, gay_r, gpy_s, gpy_r, gpx_s, gpx_r,
    saz_s, saz_r, spz_s, spz_r, say_s, say_r, spy_s, spy_r, spx_s, spx_r,
):
    outer, inner, p, s, z, y = place(pair_size, seq_size)
    f32, bf16 = jnp.float32, jnp.bfloat16
    rows_here = q_ref.shape[0]
    pairs = rows_here * batch
    answer_rows, prefix_rows = a_in.shape[2], p_in.shape[2]
    total_rows = group * rows_here
    scaling = HEAD_DIM**-0.5
    first = s * rows_here
    others = range(1, pair_size)
    mates = range(1, inner)
    line = range(1, outer)

    def shuffle(back):
        new = lax.broadcasted_iota(jnp.int32, (pairs, pairs), 1 if back else 0)
        old = lax.broadcasted_iota(jnp.int32, (pairs, pairs), 0 if back else 1)
        return (lax.rem(new, rows_here) * batch + lax.div(new, rows_here) == old).astype(f32).astype(bf16)

    def split_batch(block):
        flat = jnp.dot(shuffle(False), block.reshape(pairs, HEAD_DIM), preferred_element_type=f32).astype(bf16)
        return [flat[b * rows_here : (b + 1) * rows_here] for b in range(batch)]

    def join_batch(parts):
        flat = jnp.dot(shuffle(True), jnp.concatenate(parts, axis=0), preferred_element_type=f32).astype(bf16)
        return flat.reshape(rows_here, batch, HEAD_DIM)

    for c in range(kv_heads):
        cut = slice(c * HEAD_DIM, (c + 1) * HEAD_DIM)
        p_in[c, 0] = pk_in[:, cut]
        p_in[c, 1] = pv_in[:, cut]
        for which, source in enumerate((ak_in, av_in)):
            for b, part in enumerate(split_batch(source[:, :, cut])):
                a_in[c * batch + b, which] = part
    for slot in range(1, seq_size):

        def clear(slot=slot):
            a_g[:, slot] = jnp.zeros((a_g.shape[0],) + a_g.shape[2:], bf16)

        only(s < slot, clear)
    greet(pair_size, outer, inner, p, z, y)
    for c in range(kv_heads):
        for g in range(group):
            cut = slice((c * group + g) * HEAD_DIM, (c * group + g + 1) * HEAD_DIM)
            rows = slice(g * rows_here, (g + 1) * rows_here)
            for b, part in enumerate(split_batch(q_ref[:, :, cut])):
                q_s[c * batch + b, rows] = part
            for b, part in enumerate(split_batch(d_ref[:, :, cut])):
                d_s[c * batch + b, rows] = part
    greeted(pair_size, outer, inner)
    sends = []

    def send(src, dst, s_sem, r_sem, device, when=None):
        copy = pltpu.make_async_remote_copy(
            src_ref=src, dst_ref=dst, send_sem=s_sem, recv_sem=r_sem, device_id=device
        )
        only(when, copy.start)
        sends.append((when, copy))
        return copy

    def line_device(k):
        return {"seq": ((z + k) % outer) * inner + y}

    def mate_device(j):
        return {"seq": z * inner + (y + j) % inner}

    gpz, gaz, gpy, gay, gpx = {}, {}, {}, {}, {}

    def start_prefix(c):
        mine = p_g.at[c, p * seq_size + s]
        for k in line:
            gpz[c, k] = send(p_in.at[c], mine, gpz_s.at[c, k - 1], gpz_r.at[c, k - 1], line_device(k))
        prefix_to_mate(c, 0, p_in.at[c], s)
        prefix_to_side(c, 0, p_in.at[c], s)
        p_g[c, p * seq_size + s] = p_in[c]

    def prefix_to_mate(c, k, src, slot):
        for j in mates:
            at = (j - 1) * outer + k
            gpy[c, j, k] = send(
                src, p_g.at[c, p * seq_size + slot], gpy_s.at[c, at], gpy_r.at[c, at], mate_device(j)
            )

    def prefix_to_side(c, index, src, slot):
        for i in others:
            at = (i - 1) * seq_size + index
            gpx[c, i, index] = send(
                src,
                p_g.at[c, p * seq_size + slot],
                gpx_s.at[c, at],
                gpx_r.at[c, at],
                {"pair": (p + i) % pair_size},
            )

    def answer_to_mate(t, k, src, slot):
        for j in mates:
            at = (j - 1) * outer + k
            when = z >= k if k > 0 else y + j < inner
            gay[t, j, k] = send(src, a_g.at[t, slot], gay_s.at[t, at], gay_r.at[t, at], mate_device(j), when)

    def start_answer(t):
        for k in line:
            gaz[t, k] = send(
                a_in.at[t], a_g.at[t, s], gaz_s.at[t, k - 1], gaz_r.at[t, k - 1], line_device(k), z + k < outer
            )
        answer_to_mate(t, 0, a_in.at[t], s)
        a_g[t, s] = a_in[t]

    def pass_prefix_line(c):
        for k in line:
            slot = ((z + outer - k) % outer) * inner + y
            gpz[c, k].wait_recv()
            src = p_g.at[c, p * seq_size + slot]
            prefix_to_mate(c, k, src, slot)
            prefix_to_side(c, k, src, slot)

    def pass_answer_line(t):
        for k in line:
            slot = ((z + outer - k) % outer) * inner + y
            only(z >= k, gaz[t, k].wait_recv)
            answer_to_mate(t, k, a_g.at[t, slot], slot)

    def pass_prefix_mate(c):
        for k in range(outer):
            for j in mates:
                slot = ((z + outer - k) % outer) * inner + (y + inner - j) % inner
                gpy[c, j, k].wait_recv()
                prefix_to_side(c, j * outer + k, p_g.at[c, p * seq_size + slot], slot)

    def ready_prefix(c):
        for i in others:
            for index in range(seq_size):
                gpx[c, i, index].wait_recv()

    def ready_answer(t):
        for k in range(outer):
            for j in mates:
                only(z >= k if k > 0 else y >= j, gay[t, j, k].wait_recv)

    order = list(line) + [0]
    spx, spy, spz, say, saz = {}, {}, {}, {}, {}

    def prefix_side(c, i):
        for j in list(mates) + [0]:
            for k in order:
                slot = ((z + k) % outer) * inner + (y + j) % inner
                at = (i - 1) * seq_size + j * outer + k
                spx[c, i, j, k] = send(
                    pt_ref.at[c, i - 1, slot],
                    rx.at[c, at],
                    spx_s.at[c, at],
                    spx_r.at[c, at],
                    {"pair": (p + i) % pair_size},
                )

    def side_sum(c, j, k):
        slot = ((z + k) % outer) * inner + (y + j) % inner
        total = pt_ref[c, pair_size - 1, slot].astype(f32)
        for i in others:
            spx[c, i, j, k].wait_recv()
            total += rx[c, (i - 1) * seq_size + j * outer + k].astype(f32)
        return total

    def prefix_mate(c):
        for k in order:
            for j in mates:
                at = (j - 1) * outer + k
                sy_p[c, at] = side_sum(c, j, k).astype(bf16)
                spy[c, j, k] = send(
                    sy_p.at[c, at], ry_p.at[c, at], spy_s.at[c, at], spy_r.at[c, at], mate_device(j)
                )

    def prefix_line(c):
        for k in order:
            total = side_sum(c, 0, k)
            for j in mates:
                spy[c, j, k].wait_recv()
                total += ry_p[c, (j - 1) * outer + k].astype(f32)
            if k > 0:
                sz_p[c, k - 1] = total.astype(bf16)
                spz[c, k] = send(
                    sz_p.at[c, k - 1], rz_p.at[c, k - 1], spz_s.at[c, k - 1], spz_r.at[c, k - 1], line_device(k)
                )
            else:
                own_p[c] = total

    def prefix_end(c):
        total = own_p[c]
        for k in line:
            spz[c, k].wait_recv()
            total += rz_p[c, k - 1].astype(f32)
        columns = slice(c * HEAD_DIM, (c + 1) * HEAD_DIM)
        pk_ref[:, columns] = total[0]
        pv_ref[:, columns] = total[1]

    def answer_mate(t):
        for k in order:
            for j in mates:
                at = (j - 1) * outer + k
                slot = ((z + k) % outer) * inner + (y + j) % inner
                say[t, j, k] = send(
                    at_ref.at[t, slot], ry_a.at[t, at], say_s.at[t, at], say_r.at[t, at], mate_device(j),
                    z + k >= outer if k > 0 else y + j >= inner,
                )

    def answer_line(t):
        for k in line:

            def pass_down(k=k):
                total = at_ref[t, (z + k - outer) * inner + y].astype(f32)
                for j in mates:
                    say[t, j, k].wait_recv()
                    total += ry_a[t, (j - 1) * outer + k].astype(f32)
                sz_a[t, k - 1] = total.astype(bf16)

            only(z + k >= outer, pass_down)
            saz[t, k] = send(
                sz_a.at[t, k - 1], rz_a.at[t, k - 1], saz_s.at[t, k - 1], saz_r.at[t, k - 1], line_device(k),
                z + k >= outer,
            )
        own_a[t] = at_ref[t, s].astype(f32)
        for j in mates:

            def add_mate(j=j):
                say[t, j, 0].wait_recv()
                own_a[t] += ry_a[t, (j - 1) * outer].astype(f32)

            only(y < j, add_mate)

    def answer_end(t, c, b):
        for k in line:

            def add_line(k=k):
                saz[t, k].wait_recv()
                own_a[t] += rz_a[t, k - 1].astype(f32)

            only(z < k, add_line)
        if b < batch - 1:
            return
        columns = slice(c * HEAD_DIM, (c + 1) * HEAD_DIM)
        for which, ref in enumerate((ak_ref, av_ref)):
            ref[:, :, columns] = join_batch([own_a[c * batch + i, which].astype(bf16) for i in range(batch)])

    lane = lax.broadcasted_iota(jnp.int32, (1, total_rows), 1)
    row = lax.broadcasted_iota(jnp.int32, (total_rows, 1), 0)
    lane_place = first + lax.rem(lane, rows_here)
    row_place = first + lax.rem(row, rows_here)

    def dot(left, right, a, b):
        return lax.dot_general(left, right, (((a,), (b,)), ((), ())), preferred_element_type=f32)

    def compute(t, c, b, between, last):
        limit, length = limits[0, b], lengths[0, b]
        q, d = q_s[t], d_s[t]
        d = jnp.where(row_place < length, d.astype(f32), 0.0)
        d_t = d.T
        d = d.astype(bf16)
        work = []
        at = 0
        for i in range(pair_size):
            side = (p + 1 + i) % pair_size
            for low, high in chunks_of(seq_size, 8):
                span = (high - low) * prefix_rows
                work.append((i, low, high, side * seq_size + low, slice(at, at + span), span))
                at += span
        for low, high in chunks_of(seq_size, 4):
            span = (high - low) * answer_rows
            work.append((-1, low, high, low, slice(at, at + span), span))
            at += span

        def rows_of(i, low, high, begin, which):
            if i >= 0:
                return flat_rows(p_g[c, pl.ds(begin, high - low), which])
            return flat_rows(a_g[t, low:high, which])

        top = jnp.full((1, total_rows), FILL, f32)
        for i, low, high, begin, where, span in work:
            scores = dot(rows_of(i, low, high, begin, 0), q, 1, 1) * (scaling * math.log2(math.e))
            place_j = lax.broadcasted_iota(jnp.int32, (span, 1), 0)
            if i >= 0:
                allowed = begin * prefix_rows + place_j < limit
            else:
                allowed = begin * answer_rows + place_j <= lane_place
            scores = jnp.where(allowed, scores, FILL)
            top = jnp.maximum(top, jnp.max(scores, axis=0, keepdims=True))
            e_ref[where, :] = scores
        between(0)
        exp_total = jnp.zeros((1, total_rows), f32)
        for i, low, high, begin, where, span in work:
            e = jnp.exp2(e_ref[where, :] - top)
            exp_total = exp_total + jnp.sum(e, axis=0, keepdims=True)
            e_ref[where, :] = e
        inverse = 1.0 / exp_total
        between(1)
        attended = jnp.zeros((HEAD_DIM, total_rows), f32)
        for i, low, high, begin, where, span in work:
            probs = e_ref[where, :] * inverse
            probs_low = probs.astype(bf16)
            e_ref[where, :] = probs
            low_ref[where, :] = probs_low
            attended = attended + dot(rows_of(i, low, high, begin, 1), probs_low, 0, 0)
        attended = jnp.where(lane_place < length, attended, 0.0)
        delta = jnp.sum(d_t * attended, axis=0, keepdims=True)
        o_s[0, b] = attended.T.astype(bf16)
        between(2)
        grad = jnp.zeros((HEAD_DIM, total_rows), f32)
        for i, low, high, begin, where, span in work:
            grad_probs = dot(rows_of(i, low, high, begin, 1), d, 1, 1)
            grad_low = (e_ref[where, :] * (grad_probs - delta)).astype(bf16)
            grad = grad + dot(rows_of(i, low, high, begin, 0), grad_low, 0, 0)
            key_term = dot(grad_low, q, 1, 0) * scaling
            value_term = dot(low_ref[where, :], d, 1, 0)
            for which, term in ((0, key_term), (1, value_term)):
                if i < 0:
                    at_ref[t, low:high, which] = term.astype(bf16).reshape(high - low, answer_rows, HEAD_DIM)
                    continue
                if b > 0:
                    term = acc_ref[which, where, :] + term
                if b < batch - 1:
                    acc_ref[which, where, :] = term
                else:
                    pt_ref[c, i, low:high, which] = term.astype(bf16).reshape(
                        high - low, prefix_rows, HEAD_DIM
                    )
            if b == batch - 1 and 0 <= i < pair_size - 1 and high == seq_size:
                prefix_side(c, i + 1)
        answer_mate(t)
        o_s[1, b] = (grad * scaling).T.astype(bf16)
        if b < batch - 1:
            return
        for which, ref in enumerate((out_ref, dq_ref)):
            for g in range(group):
                cut = slice((c * group + g) * HEAD_DIM, (c * group + g + 1) * HEAD_DIM)
                rows = slice(g * rows_here, (g + 1) * rows_here)
                ref[:, :, cut] = join_batch([o_s[which, i, rows] for i in range(batch)])

    items = [(c, b) for c in range(kv_heads) for b in range(batch)]
    count = len(items)
    for t, (c, b) in enumerate(items):
        if b == 0:
            start_prefix(c)
        start_answer(t)

    def prepare(t):
        if t < count:
            if items[t][1] == 0:
                pass_prefix_line(items[t][0])
            pass_answer_line(t)

    def prepare_mate(t):
        if t < count and items[t][1] == 0:
            pass_prefix_mate(items[t][0])

    prepare(0)
    prepare_mate(0)
    prepare(1)
    for t, (c, b) in enumerate(items):
        if b == 0:
            ready_prefix(c)
        ready_answer(t)

        def between(stage, t=t, c=c, b=b):
            if stage == 0:
                prepare(t + 2)
            if stage == 1:
                if t > 0:
                    answer_line(t - 1)
                if b == 0 and c > 0:
                    prefix_mate(c - 1)
            if stage == 2:
                prepare_mate(t + 2)
                if b == 0 and c > 0:
                    prefix_line(c - 1)

        compute(t, c, b, between, t == count - 1)
    prefix_mate(kv_heads - 1)
    answer_line(count - 1)
    prefix_line(kv_heads - 1)
    for t, (c, b) in enumerate(items):
        answer_end(t, c, b)
    for c in range(kv_heads):
        prefix_end(c)
    for when, copy in sends:
        only(when, copy.wait_send)


def layer(pair_size, seq_size, batch, kv_heads, limits, lengths, q, d, ak, av, pk, pv):
    outer, inner = split_seq(seq_size)
    dma = pltpu.SemaphoreType.DMA
    low, f32 = jnp.bfloat16, jnp.float32
    rows_here, _, width = q.shape
    items = batch * kv_heads
    group = width // HEAD_DIM // kv_heads
    answer_rows, prefix_rows = ak.shape[0], pk.shape[0]
    a_one, p_one = (2, answer_rows, HEAD_DIM), (2, prefix_rows, HEAD_DIM)
    i1, o1, q1 = max(inner - 1, 1), max(outer - 1, 1), max(pair_size - 1, 1)
    prefix_keys = pair_size * seq_size * prefix_rows
    keys = prefix_keys + seq_size * answer_rows
    total_rows = group * rows_here
    semaphores = []
    for shape in 2 * (
        (items, o1), (kv_heads, o1), (items, i1 * outer), (kv_heads, i1 * outer), (kv_heads, q1 * seq_size)
    ):
        semaphores += [dma(shape), dma(shape)]
    answer_out = jax.ShapeDtypeStruct(ak.shape, low)
    prefix_out = jax.ShapeDtypeStruct((prefix_rows, kv_heads * HEAD_DIM), f32)
    return pl.pallas_call(
        functools.partial(layer_kernel, pair_size, seq_size, batch, kv_heads, group),
        out_shape=(
            jax.ShapeDtypeStruct(q.shape, low),
            jax.ShapeDtypeStruct(q.shape, low),
            answer_out, answer_out, prefix_out, prefix_out,
        ),
        in_specs=[pl.BlockSpec(memory_space=pltpu.SMEM)] * 2 + [pl.BlockSpec(memory_space=VM)] * 6,
        out_specs=(pl.BlockSpec(memory_space=VM),) * 6,
        scratch_shapes=[
            VM((items,) + a_one, low),
            VM((kv_heads,) + p_one, low),
            VM((items, seq_size) + a_one, low),
            VM((kv_heads, pair_size * seq_size) + p_one, low),
            VM((items, seq_size) + a_one, low),
            VM((kv_heads, pair_size, seq_size) + p_one, low),
            VM((keys, total_rows), f32),
            VM((keys, total_rows), low),
            VM((2, prefix_keys, HEAD_DIM), f32),
            VM((kv_heads, q1 * seq_size) + p_one, low),
            VM((kv_heads, i1 * outer) + p_one, low),
            VM((kv_heads, o1) + p_one, low),
            VM((items, i1 * outer) + a_one, low),
            VM((items, o1) + a_one, low),
            VM((kv_heads, i1 * outer) + p_one, low),
            VM((kv_heads, o1) + p_one, low),
            VM((items, o1) + a_one, low),
            VM((items,) + a_one, f32),
            VM((kv_heads,) + p_one, f32),
            VM((items, total_rows, HEAD_DIM), low),
            VM((items, total_rows, HEAD_DIM), low),
            VM((2, batch, total_rows, HEAD_DIM), low),
        ] + semaphores,
        compiler_params=pltpu.CompilerParams(
            collective_id=0, has_side_effects=True, vmem_limit_bytes=60 * 1024 * 1024
        ),
        name="attention_layer",
    )(limits, lengths, q, d, ak, av, pk, pv)


def hand_on(*refs):
    half = len(refs) // 2
    for source, target in zip(refs[:half], refs[half:]):
        target[...] = source[...]


def write_out(results):
    return pl.pallas_call(
        hand_on,
        out_shape=tuple(jax.ShapeDtypeStruct(r.shape, r.dtype) for r in results),
        in_specs=[pl.BlockSpec(memory_space=VM)] * len(results),
        out_specs=(pl.BlockSpec(memory_space=VM),) * len(results),
        compiler_params=pltpu.CompilerParams(vmem_limit_bytes=60 * 1024 * 1024),
        name="write_out",
    )(*results)


def on_device(
    pair_size,
    seq_size,
    queries,
    answer_keys,
    answer_values,
    prefix_keys,
    prefix_values,
    grad_out,
    answer_length,
    prefix_limit,
):
    _, rows, batch, width = queries.shape
    size = HEAD_DIM
    kv_heads = answer_keys.shape[3] // size
    flat = queries.shape[1:]
    flat_keys = answer_keys.shape[1:]
    out, dq, ak, av, pk, pv = write_out(layer(
        pair_size, seq_size, batch, kv_heads, prefix_limit, answer_length,
        queries.reshape(flat), grad_out.reshape(flat),
        answer_keys.reshape(flat_keys), answer_values.reshape(flat_keys), prefix_keys, prefix_values,
    ))
    return (
        out.reshape(queries.shape),
        dq.reshape(queries.shape),
        ak.reshape(answer_keys.shape),
        av.reshape(answer_values.shape),
        pk,
        pv,
    )


def solution(mesh):
    rows = P("pair", "seq", None, "head")
    prefix = P(("pair", "seq"), "head")
    return jax.shard_map(
        functools.partial(on_device, mesh.shape["pair"], mesh.shape["seq"]),
        mesh=mesh,
        in_specs=(rows, rows, rows, prefix, prefix, rows, P("pair", None), P("pair", None)),
        out_specs=(rows, rows, rows, rows, prefix, prefix),
        check_vma=False,
    )
```
